256 devices in a mesh: gp: 4 (over y, x), blk: 64 (over z, core).
Axes of the slice: x: 2, y: 2, z: 32, core: 2. Of those that a mesh axis runs over, the one named last changes fastest.
The devices are a block of a 4x8x32 slice.
Arguments:
- points: float32 [8, 65536], P(None, ('gp', 'blk')), parts along dimension 1, may hold values from -6 to 6
- vectors: float32 [8, 65536], P(None, ('gp', 'blk')), parts along dimension 1, may hold values from -6 to 6
- inv_length: float32 [32], P('gp'), parts along dimension 0, may hold values from 0.15 to 0.6
- noise: float32 [4], P('gp'), parts along dimension 0, may hold values from 0.1 to 1
Outputs:
- product: float32 [8, 65536], P(None, ('gp', 'blk')), parts along dimension 1
The draws below stay inside these ranges and needn't reach their ends.
There are 4 independent parts, one for each index of `gp`. The reference program is written for one: setup_inputs(seed, part) draws one part's arguments, and reference() takes and returns one part's arrays. A program takes and returns all parts, laid end to end along the dimension named above; each array names one. Nothing has to cross between parts.
All inputs are finite; a program needn't handle non-finite values.
Results may differ from the reference program's by a relative error of at most 0.00017.
Values sent between devices are 32-bit elements; how exact they have to be, the bound alone decides.
A program may use at most 64 MiB of HBM per device.

```python
import math
import jax
import jax.numpy as jnp
from jax import lax

DIM = 8
RHS = 8
PTS_DEV = 256
NPTS = 16384


def block_levels(stream_key, extent, pieces, low, high):
    factor_of, own = 1.0, jax.random.fold_in(stream_key, 6)
    for position, shards_of in pieces:
        draws = jnp.exp(jax.random.uniform(jax.random.fold_in(own, position), (shards_of,), jnp.float32, low / len(pieces), high / len(pieces)))
        factor_of = factor_of * jnp.repeat(draws, extent[position] // shards_of).reshape([-1 if axis == position else 1 for axis in range(len(extent))])
    return factor_of


def centred(key, extent, spread, bound, shards=(), kind=jnp.bfloat16):
    loudness = block_levels(key, extent, shards, -0.22, 0.18) if shards else 1.0
    values = jax.random.normal(key, extent, jnp.float32) * spread * loudness
    return jnp.minimum(jnp.maximum(values, -bound), bound).astype(kind)


def setup_inputs(seed: int = 0, part: int = 0) -> dict:
    key_list = jax.random.split(jax.random.key(seed), 5)
    own_keys = jax.random.split(jax.random.fold_in(key_list[4], part), 5)
    points = centred(own_keys[0], (DIM, NPTS), 1.0, 6.0, ((1, 64),), jnp.float32)
    vectors = centred(own_keys[1], (RHS, NPTS), 1.0, 6.0, ((1, 64),), jnp.float32)
    inv_length = jnp.clip(jnp.exp(jax.random.uniform(own_keys[2], (DIM,), jnp.float32, math.log(0.15), math.log(0.6))), 0.15, 0.6)
    noise = jnp.clip(jnp.exp(jax.random.uniform(own_keys[3], (1,), jnp.float32, math.log(0.1), math.log(1.0))), 0.1, 1.0)
    return {"points": points, "vectors": vectors, "inv_length": inv_length, "noise": noise}


def matern(left, right, inv_length):
    scaled_left = left * inv_length[:, None]
    scaled_right = right * inv_length[:, None]
    sq_left = lax.optimization_barrier(jnp.sum(scaled_left * scaled_left, axis=0))
    sq_right = lax.optimization_barrier(jnp.sum(scaled_right * scaled_right, axis=0))
    cross = jnp.dot(scaled_left.T, scaled_right, precision=lax.Precision.HIGHEST, preferred_element_type=jnp.float32)
    dist2 = jnp.maximum(sq_left[:, None] + sq_right[None, :] - 2.0 * cross, 0.0)
    scaled_dist = jnp.sqrt(5.0 * dist2)
    return (1.0 + scaled_dist + scaled_dist * scaled_dist / 3.0) * jnp.exp(-scaled_dist)

def reference(points, vectors, inv_length, noise):
    blocks = points.reshape(DIM, NPTS // PTS_DEV, PTS_DEV).transpose(1, 0, 2)

    def one_block(block):
        tile = matern(points, block, inv_length)
        return jnp.dot(vectors, tile, precision=lax.Precision.HIGHEST, preferred_element_type=jnp.float32)
    sums = lax.map(one_block, blocks)
    sums = sums.transpose(1, 0, 2).reshape(RHS, NPTS)
    return noise[0] * vectors + sums / jnp.sqrt(jnp.float32(NPTS))
```

```python
import functools
import math

import jax
import jax.numpy as jnp
from jax import lax
from jax.experimental import pallas as pl
from jax.experimental.pallas import tpu as pltpu
from jax.sharding import PartitionSpec as P

NEAR = 8
ROWS = 128
LN2 = math.log(2.0)
UNIT = LN2 * LN2 / 3.0
TINY = 1e-30
MESH = pl.DeviceIdType.MESH
F32, BF16 = jnp.float32, jnp.bfloat16


def split(x, count):
    parts = []
    for _ in range(count):
        part = x.astype(BF16).astype(F32)
        parts.append(part)
        x = x - part
    return parts


def factors(scaled):
    sq = jnp.sum(scaled * scaled, axis=0, keepdims=True)
    hi, mid, low = split(scaled, 3)
    sq_parts = split(sq, 3)
    row = lax.broadcasted_iota(jnp.int32, scaled.shape, 0)
    first = jnp.where(row == 0, sq_parts[0], jnp.where(row == 1, sq_parts[1], jnp.where(row == 2, sq_parts[2], 0.0)))
    left_sq = jnp.where((row >= 3) & (row < 6), 1.0, first)
    second = jnp.where(row == 3, sq_parts[0], jnp.where(row == 4, sq_parts[1], jnp.where(row == 5, sq_parts[2], 0.0)))
    right_sq = jnp.where(row < 3, 1.0, second)
    return [hi, hi, mid, hi, low, mid, left_sq], [-2.0 * hi, -2.0 * mid, -2.0 * hi, -2.0 * low, -2.0 * hi, -2.0 * mid, right_sq]


def put_rows(points, inv, left_ref, start):
    left, _ = factors(points * inv)
    left = jnp.concatenate(left + [jnp.zeros_like(points)], axis=0)
    left_ref[pl.ds(start, points.shape[1]), :] = left.T.astype(BF16)


def add_block(block_ref, inv, left_ref, acc_ref):
    dim = block_ref.shape[0] // 2
    points, vectors = block_ref[:dim, :], block_ref[dim:, :]
    _, right = factors(points * inv)
    right = jnp.concatenate(right + [jnp.zeros_like(points)], axis=0).astype(BF16)
    vec_parts = jnp.concatenate(split(vectors, 2), axis=0).astype(BF16)
    vec_parts = jnp.concatenate([vec_parts, vec_parts], axis=1)
    for start in range(0, left_ref.shape[0], ROWS):
        rows = pl.ds(start, ROWS)
        squared = jnp.maximum(jnp.dot(left_ref[rows, :], right, preferred_element_type=F32), TINY)
        dist = squared * lax.rsqrt(squared)
        kern = (dist * (dist + 3.0 / LN2) + 3.0 / (LN2 * LN2)) * jnp.exp2(-dist)
        high = kern.astype(BF16)
        low = (kern - high.astype(F32)).astype(BF16)
        both = jnp.concatenate([high, low], axis=1)
        added = lax.dot_general(both, vec_parts, (((1,), (1,)), ((), ())), preferred_element_type=F32)
        acc_ref[rows, :] = acc_ref[rows, :] + added


def kernel(
    count, inv_ref, points_ref, vectors_ref, out_ref,
    blocks, near, left_ref, acc_ref, sums, sums_in,
    own_sem, far_send, far_recv, near_send, near_recv, sum_send, sum_recv,
):
    me = lax.axis_index("blk")
    member = lax.rem(me, NEAR)
    base = me - member
    dim, points = points_ref.shape
    above, below = lax.rem(me + NEAR, count), lax.rem(me + count - NEAR, count)
    ups = count // NEAR // 2
    downs = count // NEAR - 1 - ups

    own = [
        pltpu.make_async_copy(points_ref, blocks.at[0, pl.ds(0, dim)], own_sem.at[0]),
        pltpu.make_async_copy(vectors_ref, blocks.at[0, pl.ds(dim, dim)], own_sem.at[1]),
        pltpu.make_async_copy(points_ref, near.at[member], own_sem.at[2]),
    ]
    for copy in own:
        copy.start()

    def other(k):
        return base + lax.rem(member + k, NEAR)

    barrier = pltpu.get_barrier_semaphore()
    for peer in [above, below] + [other(k) for k in range(1, NEAR)]:
        pl.semaphore_signal(barrier, inc=1, device_id={"blk": peer}, device_id_type=MESH)

    def remote(source, target, sends, recvs, i_send, i_recv, peer):
        return pltpu.make_async_remote_copy(
            src_ref=source, dst_ref=target, send_sem=sends.at[i_send], recv_sem=recvs.at[i_recv],
            device_id={"blk": peer}, device_id_type=MESH,
        )

    def up(k):
        return remote(blocks.at[k - 1], blocks.at[k], far_send, far_recv, k, k, above)

    def down(k):
        source = 0 if k == 1 else ups + k - 1
        return remote(blocks.at[source], blocks.at[ups + k], far_send, far_recv, ups + k, ups + k, below)

    def points_to(k):
        return remote(blocks.at[0, pl.ds(0, dim)], near.at[member], near_send, near_recv, k, member, other(k))

    def points_from(k):
        return remote(blocks.at[0, pl.ds(0, dim)], near.at[other(k) - base], near_send, near_recv, k, other(k) - base, other(k))

    def sums_to(k):
        return remote(sums.at[other(k) - base], sums_in.at[member], sum_send, sum_recv, k, member, other(k))

    def sums_from(k):
        return remote(sums.at[0], sums_in.at[other(k) - base], sum_send, sum_recv, k, other(k) - base, other(k))

    row = lax.broadcasted_iota(jnp.int32, (dim, points), 0)
    inv = jnp.zeros((dim, points), F32)
    for d in range(dim):
        inv = jnp.where(row == d, inv_ref[d] * (math.sqrt(5.0) / LN2), inv)
    acc_ref[...] = jnp.zeros_like(acc_ref)

    for copy in own:
        copy.wait()
    pl.semaphore_wait(barrier, NEAR + 1)
    up(1).start()
    down(1).start()
    for k in range(1, NEAR):
        points_to(k).start()
    for k in range(1, NEAR):
        points_from(k).wait_recv()

    @pl.loop(0, NEAR)
    def _(m):
        put_rows(near[m], inv, left_ref, pl.multiple_of(m * points, points))

    @pl.loop(0, count // NEAR)
    def _(step):
        for k in range(1, ups + 1):
            @pl.when(step == (2 * k - 3 if k > 1 else 0) if k < ups or downs == ups else step == 2 * k - 1)
            def _():
                up(k).wait_recv()
                if k < ups:
                    up(k + 1).start()
                if k <= downs:
                    down(k).wait_recv()
                    if k < downs:
                        down(k + 1).start()

        stage = (step + 1) // 2
        slot = jnp.where((step > 0) & (lax.rem(step, 2) == 0), ups + stage, stage)
        add_block(blocks.at[slot], inv, left_ref, acc_ref)

    @pl.loop(0, NEAR)
    def _(m):
        both = acc_ref[pl.ds(pl.multiple_of(m * points, points), points), :].T
        sums[m] = both[:dim] + both[dim:]

    for k in range(1, NEAR):
        sums_to(k).start()
    sums_in[member] = sums[member]
    for k in range(1, NEAR):
        sums_from(k).wait_recv()
    total = sums_in[0]
    for m in range(1, NEAR):
        total = total + sums_in[m]
    out_ref[...] = total

    for k in range(1, ups + 1):
        up(k).wait_send()
    for k in range(1, downs + 1):
        down(k).wait_send()
    for k in range(1, NEAR):
        points_to(k).wait_send()
        sums_to(k).wait_send()


def on_device(points, vectors, inv_length, noise):
    count = lax.axis_size("blk")
    dim, size = points.shape
    rhs = vectors.shape[0]
    groups = count // NEAR
    total = pl.pallas_call(
        functools.partial(kernel, count),
        out_shape=jax.ShapeDtypeStruct(vectors.shape, F32),
        in_specs=[
            pl.BlockSpec(memory_space=pltpu.SMEM),
            pl.BlockSpec(memory_space=pl.ANY),
            pl.BlockSpec(memory_space=pl.ANY),
        ],
        out_specs=pl.BlockSpec(memory_space=pltpu.VMEM),
        scratch_shapes=[
            pltpu.VMEM((groups, dim + rhs, size), F32),
            pltpu.VMEM((NEAR, dim, size), F32),
            pltpu.VMEM((NEAR * size, 8 * dim), BF16),
            pltpu.VMEM((NEAR * size, 2 * rhs), F32),
            pltpu.VMEM((NEAR, rhs, size), F32),
            pltpu.VMEM((NEAR, rhs, size), F32),
            pltpu.SemaphoreType.DMA((3,)),
            pltpu.SemaphoreType.DMA((groups,)),
            pltpu.SemaphoreType.DMA((groups,)),
            pltpu.SemaphoreType.DMA((NEAR,)),
            pltpu.SemaphoreType.DMA((NEAR,)),
            pltpu.SemaphoreType.DMA((NEAR,)),
            pltpu.SemaphoreType.DMA((NEAR,)),
        ],
        compiler_params=pltpu.CompilerParams(collective_id=0, has_side_effects=True),
        name="matern_product",
    )(inv_length, points, vectors)
    return noise[0] * vectors + total * (UNIT / math.sqrt(size * count))


def solution(mesh):
    return jax.shard_map(
        on_device,
        mesh=mesh,
        in_specs=(P(None, ("gp", "blk")), P(None, ("gp", "blk")), P("gp"), P("gp")),
        out_specs=P(None, ("gp", "blk")),
        check_vma=False,
    )
```

```python
import functools
import math

import jax
import jax.numpy as jnp
from jax import lax
from jax.experimental import pallas as pl
from jax.experimental.pallas import tpu as pltpu
from jax.sharding import PartitionSpec as P

NEAR = 8
COLS = 256
LN2 = math.log(2.0)
UNIT = 3.0
TINY = 1e-30
MESH = pl.DeviceIdType.MESH
F32, BF16 = jnp.float32, jnp.bfloat16


def split(x, count):
    parts = []
    for _ in range(count):
        part = x.astype(BF16).astype(F32)
        parts.append(part)
        x = x - part
    return parts


def factors(scaled):
    sq = jnp.sum(scaled * scaled, axis=0, keepdims=True)
    hi, mid, low = split(scaled, 3)
    sq_parts = split(sq, 3)
    row = lax.broadcasted_iota(jnp.int32, scaled.shape, 0)
    first = jnp.where(row == 0, sq_parts[0], jnp.where(row == 1, sq_parts[1], jnp.where(row == 2, sq_parts[2], 0.0)))
    left_sq = jnp.where((row >= 3) & (row < 6), 1.0, first)
    second = jnp.where(row == 3, sq_parts[0], jnp.where(row == 4, sq_parts[1], jnp.where(row == 5, sq_parts[2], 0.0)))
    right_sq = jnp.where(row < 3, 1.0, second)
    return [hi, hi, mid, hi, low, mid, left_sq], [-2.0 * hi, -2.0 * mid, -2.0 * hi, -2.0 * low, -2.0 * hi, -2.0 * mid, right_sq]


def put_columns(points, inv, right_ref, start):
    _, right = factors(points * inv)
    right_ref[:, pl.ds(start, points.shape[1])] = jnp.concatenate(right + [jnp.zeros_like(points)], axis=0).astype(BF16)


def add_blocks(block_refs, inv, right_ref, acc_ref):
    lefts, vecs = [], []
    for block_ref in block_refs:
        dim = block_ref.shape[0] // 2
        left, _ = factors(block_ref[:dim, :] * inv)
        lefts.append(jnp.concatenate(left + [jnp.zeros_like(inv)], axis=0).T.astype(BF16))
        vecs.append(jnp.concatenate(split(block_ref[dim:, :], 2), axis=0).astype(BF16))
    for start in range(0, right_ref.shape[1], COLS):
        cols = pl.ds(start, COLS)
        added = acc_ref[:, cols]
        for left, vec in zip(lefts, vecs):
            squared = jnp.maximum(jnp.dot(left, right_ref[:, cols], preferred_element_type=F32), TINY)
            dist = squared * lax.rsqrt(squared)
            kern = (squared + dist + 1.0 / 3.0) * jnp.exp2(dist * (-3.0 / LN2))
            high = kern.astype(BF16)
            low = (kern - high.astype(F32)).astype(BF16)
            added = added + jnp.dot(vec, high, preferred_element_type=F32)
            added = added + jnp.dot(vec, low, preferred_element_type=F32)
        acc_ref[:, cols] = added


def kernel(
    count, inv_ref, points_ref, vectors_ref, out_ref,
    blocks, near, right_ref, acc_ref, sums, sums_in,
    own_sem, far_send, far_recv, near_send, near_recv, sum_send, sum_recv,
):
    me = lax.axis_index("blk")
    member = lax.rem(me, NEAR)
    base = me - member
    dim, points = points_ref.shape
    above, below = lax.rem(me + NEAR, count), lax.rem(me + count - NEAR, count)
    ups = count // NEAR // 2
    downs = count // NEAR - 1 - ups

    own = [
        pltpu.make_async_copy(points_ref, blocks.at[0, pl.ds(0, dim)], own_sem.at[0]),
        pltpu.make_async_copy(vectors_ref, blocks.at[0, pl.ds(dim, dim)], own_sem.at[1]),
        pltpu.make_async_copy(points_ref, near.at[member], own_sem.at[2]),
    ]
    for copy in own:
        copy.start()

    def other(k):
        return base + lax.rem(member + k, NEAR)

    barrier = pltpu.get_barrier_semaphore()
    for peer in [above, below] + [other(k) for k in range(1, NEAR)]:
        pl.semaphore_signal(barrier, inc=1, device_id={"blk": peer}, device_id_type=MESH)

    def remote(source, target, sends, recvs, i_send, i_recv, peer):
        return pltpu.make_async_remote_copy(
            src_ref=source, dst_ref=target, send_sem=sends.at[i_send], recv_sem=recvs.at[i_recv],
            device_id={"blk": peer}, device_id_type=MESH,
        )

    def up(k):
        return remote(blocks.at[k - 1], blocks.at[k], far_send, far_recv, k, k, above)

    def down(k):
        source = 0 if k == 1 else ups + k - 1
        return remote(blocks.at[source], blocks.at[ups + k], far_send, far_recv, ups + k, ups + k, below)

    def points_to(k):
        return remote(blocks.at[0, pl.ds(0, dim)], near.at[member], near_send, near_recv, k, member, other(k))

    def points_from(k):
        return remote(blocks.at[0, pl.ds(0, dim)], near.at[other(k) - base], near_send, near_recv, k, other(k) - base, other(k))

    def sums_to(k):
        return remote(sums.at[other(k) - base], sums_in.at[member], sum_send, sum_recv, k, member, other(k))

    def sums_from(k):
        return remote(sums.at[0], sums_in.at[other(k) - base], sum_send, sum_recv, k, other(k) - base, other(k))

    row = lax.broadcasted_iota(jnp.int32, (dim, points), 0)
    inv = jnp.zeros((dim, points), F32)
    for d in range(dim):
        inv = jnp.where(row == d, inv_ref[d] * (math.sqrt(5.0) / 3.0), inv)
    acc_ref[...] = jnp.zeros_like(acc_ref)

    for copy in own:
        copy.wait()
    pl.semaphore_wait(barrier, NEAR + 1)
    up(1).start()
    down(1).start()
    for k in range(1, NEAR):
        points_to(k).start()
    for k in range(1, NEAR):
        points_from(k).wait_recv()

    @pl.loop(0, NEAR)
    def _(m):
        put_columns(near[m], inv, right_ref, pl.multiple_of(m * points, points))

    def pass_on(k):
        up(k).wait_recv()
        if k < ups:
            up(k + 1).start()
        if k <= downs:
            down(k).wait_recv()
            if k < downs:
                down(k + 1).start()

    if downs > 0:
        pass_on(1)
    add_blocks([blocks.at[0]], inv, right_ref, acc_ref)

    @pl.loop(1, downs + 1)
    def _(stage):
        for k in range(2, downs + 1):
            @pl.when(stage == k - 1)
            def _():
                pass_on(k)
        add_blocks([blocks.at[stage], blocks.at[ups + stage]], inv, right_ref, acc_ref)

    if ups > downs:
        pass_on(ups)
        add_blocks([blocks.at[ups]], inv, right_ref, acc_ref)

    for m in range(NEAR):
        both = acc_ref[:, pl.ds(m * points, points)]
        sums[m] = both[:dim] + both[dim:]

    for k in range(1, NEAR):
        sums_to(k).start()
    sums_in[member] = sums[member]
    for k in range(1, NEAR):
        sums_from(k).wait_recv()
    total = sums_in[0]
    for m in range(1, NEAR):
        total = total + sums_in[m]
    out_ref[...] = total

    for k in range(1, ups + 1):
        up(k).wait_send()
    for k in range(1, downs + 1):
        down(k).wait_send()
    for k in range(1, NEAR):
        points_to(k).wait_send()
        sums_to(k).wait_send()


def on_device(points, vectors, inv_length, noise):
    count = lax.axis_size("blk")
    dim, size = points.shape
    rhs = vectors.shape[0]
    groups = count // NEAR
    total = pl.pallas_call(
        functools.partial(kernel, count),
        out_shape=jax.ShapeDtypeStruct(vectors.shape, F32),
        in_specs=[
            pl.BlockSpec(memory_space=pltpu.SMEM),
            pl.BlockSpec(memory_space=pl.ANY),
            pl.BlockSpec(memory_space=pl.ANY),
        ],
        out_specs=pl.BlockSpec(memory_space=pltpu.VMEM),
        scratch_shapes=[
            pltpu.VMEM((groups, dim + rhs, size), F32),
            pltpu.VMEM((NEAR, dim, size), F32),
            pltpu.VMEM((8 * dim, NEAR * size), BF16),
            pltpu.VMEM((2 * rhs, NEAR * size), F32),
            pltpu.VMEM((NEAR, rhs, size), F32),
            pltpu.VMEM((NEAR, rhs, size), F32),
            pltpu.SemaphoreType.DMA((3,)),
            pltpu.SemaphoreType.DMA((groups,)),
            pltpu.SemaphoreType.DMA((groups,)),
            pltpu.SemaphoreType.DMA((NEAR,)),
            pltpu.SemaphoreType.DMA((NEAR,)),
            pltpu.SemaphoreType.DMA((NEAR,)),
            pltpu.SemaphoreType.DMA((NEAR,)),
        ],
        compiler_params=pltpu.CompilerParams(collective_id=0, has_side_effects=True),
        name="matern_product",
    )(inv_length, points, vectors)
    return noise[0] * vectors + total * (UNIT / math.sqrt(size * count))


def solution(mesh):
    return jax.shard_map(
        on_device,
        mesh=mesh,
        in_specs=(P(None, ("gp", "blk")), P(None, ("gp", "blk")), P("gp"), P("gp")),
        out_specs=P(None, ("gp", "blk")),
        check_vma=False,
    )
```
